32 devices in a mesh: row: 8 (over z, y), col: 4 (over x, core).
Axes of the slice: x: 2, y: 2, z: 4, core: 2. Of those that a mesh axis runs over, the one named last changes fastest.
Arguments:
- front: float32 [4096, 65536], P('row', 'col'), may hold values from -1 to 1
- omega: float32 [65536, 640], P(('col', 'row')), may hold values from -6 to 6
- leaf_pivots: int32 [16, 128], P('row'), may hold values from 0 to 255, as said below
- pivots_one: int32 [8, 128], P('row'), may hold values from 0 to 255, as said below
- pivots_two: int32 [4, 128], replicated, may hold values from 0 to 255, as said below
- pivots_three: int32 [2, 128], replicated, may hold values from 0 to 255, as said below
- pivots_four: int32 [1, 128], replicated, may hold values from 0 to 255, as said below
Outputs:
- samples: float32 [4096, 640], P('row')
- leaf_basis: float32 [16, 256, 128], P('row')
- basis_one: float32 [8, 256, 128], P('row')
- basis_two: float32 [8, 256, 128], P('row')
- basis_three: float32 [8, 256, 128], P('row')
- basis_four: float32 [8, 256, 128], P('row')
The draws below stay inside these ranges and needn't reach their ends.
Inputs may be any that keep to these rules, and one draw needn't show every extreme that they name: `leaf_pivots`: each row holds 128 distinct indices. `pivots_one`: each row holds 128 distinct indices. `pivots_two`: each row holds 128 distinct indices. `pivots_three`: each row holds 128 distinct indices. `pivots_four`: each row holds 128 distinct indices.
All inputs are finite; a program needn't handle non-finite values.
Results may differ from the reference program's by a relative error of at most 0.0003.
Values sent between devices are 32-bit elements; how exact they have to be, the bound alone decides.
A program may use at most 128 MiB of HBM per device.

```python
import math
import jax
import jax.numpy as jnp
from jax import lax

N = 65536
SAMPLES = 640
LEAF = 256
RANK = 128
ROWS = 4096
LEAVES = 16
N_ROW = 8


def walsh_matrix(order):
    indices = jnp.arange(order, dtype=jnp.int32)
    common_bits = indices[:, None] & indices[None, :]
    parity = jnp.zeros((order, order), jnp.int32)
    for position in range(max(order.bit_length(), 1)):
        parity = parity + (common_bits >> position & 1)
    return (1 - 2 * (parity % 2)).astype(jnp.float32) / math.sqrt(order)


def draw_front(key, part):
    mixing = walsh_matrix(LEAF)
    smallest_grade = 0.05
    ramp = jnp.arange(LEAF, dtype=jnp.float32) / (LEAF - 1)
    grades = jnp.power(jnp.float32(smallest_grade), ramp)
    grades = grades / jnp.sqrt(jnp.mean(grades * grades))
    base_key = jax.random.fold_in(key, 21)

    def one_leaf(number):
        leaf_key = jax.random.fold_in(base_key, number)
        noise_key, sign_key = jax.random.split(leaf_key)
        noise = jax.random.truncated_normal(noise_key, -6.0, 6.0, (LEAF, N), jnp.float32)
        signs = (1 - 2 * jax.random.randint(sign_key, (LEAF,), 0, 2)).astype(jnp.float32)
        mixed = jnp.dot(mixing, grades[:, None] * noise, precision=lax.Precision.HIGHEST, preferred_element_type=jnp.float32)
        return jnp.clip(signs[:, None] * mixed / math.sqrt(N), -1.0, 1.0)
    leaves = lax.map(one_leaf, jnp.arange(LEAVES, dtype=jnp.int32))
    return leaves.reshape(ROWS, N).astype(jnp.float32)


def choose_rows(key, count):
    keys = jax.random.split(key, count)
    picked = jax.vmap(lambda k: jax.random.permutation(k, LEAF)[:RANK])(keys)
    return picked.astype(jnp.int32)


def draw_leaf_pivots(key, part):
    return choose_rows(jax.random.fold_in(key, 11), LEAVES)


def draw_pivots_one(key, part):
    return choose_rows(jax.random.fold_in(key, 12), N_ROW)


def draw_pivots_two(key, part):
    return choose_rows(jax.random.fold_in(key, 13), N_ROW // 2)


def draw_pivots_three(key, part):
    return choose_rows(jax.random.fold_in(key, 14), N_ROW // 4)


def draw_pivots_four(key, part):
    return choose_rows(jax.random.fold_in(key, 15), N_ROW // 8)


def block_levels(own_key, dims, pieces, low, top_value):
    factor_of = 1.0
    for dim, parts in pieces:
        draws = jax.random.uniform(jax.random.fold_in(jax.random.fold_in(own_key, 6), dim), (parts,), jnp.float32, low / len(pieces), top_value / len(pieces))
        factor_of = factor_of * jnp.repeat(jnp.exp(draws), dims[dim] // parts).reshape((-1,) + (1,) * (len(dims) - 1 - dim))
    return factor_of


def gaussian(stream_key, dims, spread, reach, cuts=(), kind=jnp.bfloat16):
    result = jax.random.normal(stream_key, dims, jnp.float32) * spread
    if len(cuts) > 0:
        result = block_levels(stream_key, dims, cuts, -0.22, 0.18) * result
    return jnp.clip(result, min=-reach, max=reach).astype(kind)


def setup_inputs(seed: int = 0) -> dict:
    arg_keys = jax.random.split(jax.random.key(seed), 8)
    front = draw_front(jax.random.fold_in(arg_keys[7], 71), 0)
    omega = gaussian(arg_keys[1], (N, SAMPLES), 1.0, 6.0, ((0, 32),), jnp.float32)
    leaf_pivots = draw_leaf_pivots(jax.random.fold_in(arg_keys[7], 71), 0)
    pivots_one = draw_pivots_one(jax.random.fold_in(arg_keys[7], 71), 0)
    pivots_two = draw_pivots_two(jax.random.fold_in(arg_keys[7], 71), 0)
    pivots_three = draw_pivots_three(jax.random.fold_in(arg_keys[7], 71), 0)
    pivots_four = draw_pivots_four(jax.random.fold_in(arg_keys[7], 71), 0)
    return {"front": front, "omega": omega, "leaf_pivots": leaf_pivots, "pivots_one": pivots_one, "pivots_two": pivots_two, "pivots_three": pivots_three, "pivots_four": pivots_four}


ridge = 1.0

def interpolate(block, pivots):
    chosen = jnp.take(block, pivots, axis=0)
    gram = jnp.dot(chosen.astype(jnp.float32), chosen.T.astype(jnp.float32), precision=lax.Precision.HIGHEST, preferred_element_type=jnp.float32)
    gram = gram + ridge * jnp.eye(gram.shape[0], dtype=jnp.float32)
    cross = jnp.dot(block.astype(jnp.float32), chosen.T.astype(jnp.float32), precision=lax.Precision.HIGHEST, preferred_element_type=jnp.float32)
    factor = jnp.linalg.cholesky(gram)
    basis = jax.scipy.linalg.cho_solve((factor, True), cross.T).T
    return (basis, chosen)

def reference(front, omega, leaf_pivots, pivots_one, pivots_two, pivots_three, pivots_four):
    samples = jnp.dot(front.astype(jnp.float32), omega.astype(jnp.float32), precision=lax.Precision.HIGHEST, preferred_element_type=jnp.float32)
    blocks = samples.reshape(LEAVES, LEAF, SAMPLES)
    leaf_basis, skeleton = jax.vmap(interpolate)(blocks, leaf_pivots)
    outs = []
    for pivots in (pivots_one, pivots_two, pivots_three, pivots_four):
        blocks = skeleton.reshape(pivots.shape[0], LEAF, SAMPLES)
        basis, skeleton = jax.vmap(interpolate)(blocks, pivots)
        outs.append(basis)
    basis_two = jnp.repeat(outs[1], 2, axis=0)
    basis_three = jnp.repeat(outs[2], 4, axis=0)
    basis_four = jnp.repeat(outs[3], 8, axis=0)
    return (samples, leaf_basis, outs[0], basis_two, basis_three, basis_four)
```

```python
import functools

import jax
import jax.numpy as jnp
from jax import lax
from jax.experimental import pallas as pl
from jax.experimental.pallas import tpu as pltpu
from jax.sharding import PartitionSpec as P

ridge = 1.0
MESH = pl.DeviceIdType.MESH
HIGHEST = lax.Precision.HIGHEST


def gather_matmul_kernel(
    n, depth, pieces, front_ref, omega_ref, out_ref, held, cols, own_sem, front_sem, send_sem, recv_sem
):
    half_ring = n // 2
    piece = depth // (2 * pieces)
    me = lax.axis_index("row")
    a, b = me // 2, me % 2
    spot = a + b * (n - 1 - 2 * a)

    def owner(place):
        place = (place + 2 * n) % n
        q = place // half_ring
        return 2 * (place + q * (n - 1 - 2 * place)) + q

    targets = (owner(spot + 1), owner(spot - 1))

    barrier = pltpu.get_barrier_semaphore()
    for target in targets:
        pl.semaphore_signal(barrier, inc=1, device_id={"row": target}, device_id_type=MESH)
    pl.semaphore_wait(barrier, 2)

    def rows_of(way, p):
        return pl.ds((way * pieces + p) * piece, piece)

    def source(step, way):
        return owner(spot - step) if way == 0 else owner(spot + step)

    def send(src, block, step, way, p):
        pltpu.make_async_remote_copy(
            src_ref=src,
            dst_ref=held.at[block, rows_of(way, p)],
            send_sem=send_sem.at[step, way, p],
            recv_sem=recv_sem.at[step, way, p],
            device_id={"row": targets[way]},
            device_id_type=MESH,
        ).start()

    def arrival(step, way, p):
        block = source(step + 1, way)
        rows = held.at[block, rows_of(way, p)]
        return pltpu.make_async_remote_copy(
            src_ref=rows,
            dst_ref=rows,
            send_sem=send_sem.at[step, way, p],
            recv_sem=recv_sem.at[step, way, p],
            device_id={"row": targets[way]},
            device_id_type=MESH,
        )

    def front_copy(block, way, p, slot):
        start = pl.multiple_of(block * depth + (way * pieces + p) * piece, piece)
        return pltpu.make_async_copy(
            front_ref.at[:, pl.ds(start, piece)], cols.at[slot], front_sem.at[slot]
        )

    for p in range(pieces):
        for way in range(2):
            send(omega_ref.at[rows_of(way, p)], me, 0, way, p)
    own = pltpu.make_async_copy(omega_ref, held.at[me], own_sem)
    own.start()
    for way in range(2):
        front_copy(me, way, 0, way).start()
    out_ref[...] = jnp.zeros_like(out_ref)
    own.wait()

    rows_tile = 256

    def multiply(block, way, p):
        @pl.loop(0, out_ref.shape[0] // rows_tile)
        def _(i):
            tile = pl.ds(pl.multiple_of(i * rows_tile, rows_tile), rows_tile)
            out_ref[tile, :] += jnp.dot(
                cols[way, tile, :],
                held[block, rows_of(way, p), :],
                precision=HIGHEST,
                preferred_element_type=jnp.float32,
            )

    def consume(step, p):
        for way in range(2):
            block = source(step, way)
            front_copy(block, way, p, way).wait()
            multiply(block, way, p)
            if p + 1 < pieces:
                front_copy(block, way, p + 1, way).start()
            else:

                @pl.when(step < n - 1)
                def _():
                    front_copy(source(step + 1, way), way, 0, way).start()

    for p in range(pieces):
        consume(0, p)

    @pl.loop(0, n - 1)
    def _(step):
        for p in range(pieces):
            for way in range(2):
                arrival(step, way, p).wait_recv()

                @pl.when(step < n - 2)
                def _():
                    block = source(step + 1, way)
                    send(held.at[block, rows_of(way, p)], block, step + 1, way, p)

            consume(step + 1, p)

    @pl.loop(0, n - 1)
    def _(step):
        for p in range(pieces):
            for way in range(2):
                arrival(step, way, p).wait_send()


def gather_matmul(front, omega, n):
    rows = front.shape[0]
    depth, width = omega.shape
    pieces = max(1, min(2, depth // 256))
    piece = depth // (2 * pieces)
    return pl.pallas_call(
        functools.partial(gather_matmul_kernel, n, depth, pieces),
        out_shape=jax.ShapeDtypeStruct((rows, width), jnp.float32),
        in_specs=[pl.BlockSpec(memory_space=pl.ANY)] * 2,
        out_specs=pl.BlockSpec(memory_space=pltpu.VMEM),
        scratch_shapes=[
            pltpu.VMEM((n, depth, width), jnp.float32),
            pltpu.VMEM((2, rows, piece), jnp.float32),
            pltpu.SemaphoreType.DMA,
            pltpu.SemaphoreType.DMA((2,)),
            pltpu.SemaphoreType.DMA((n - 1, 2, pieces)),
            pltpu.SemaphoreType.DMA((n - 1, 2, pieces)),
        ],
        compiler_params=pltpu.CompilerParams(
            collective_id=0, has_side_effects=True, vmem_limit_bytes=60 * 1024 * 1024
        ),
    )(front, omega)


def interpolate_kernel(problems, samples, merged, b2, b3, b4, s1, s2, s3, s4, *rest):
    leaf_out, *outs = rest[:5]
    inverse = rest[5]
    leaves = leaf_out.shape[0]
    block_rows, rank = leaf_out.shape[1:]
    pairs = []
    for leaf in range(leaves):
        pairs.append(
            (
                samples.at[pl.ds(leaf * block_rows, block_rows)],
                merged.at[pl.ds(leaf * rank, rank)],
                leaf_out.at[leaf],
            )
        )
    for block, chosen, out in zip((merged, b2, b3, b4), (s1, s2, s3, s4), outs):
        pairs.append((block, chosen, out.at[0]))

    def outer(x, y):
        return lax.dot_general(
            x, y, (((1,), (1,)), ((), ())), precision=HIGHEST, preferred_element_type=jnp.float32
        )

    lane = lax.broadcasted_iota(jnp.int32, (rank, rank), 1)
    sub = lax.broadcasted_iota(jnp.int32, (rank, rank), 0)
    for j, (block, chosen, out) in enumerate(pairs):
        gram = outer(chosen[...], chosen[...])
        inverse[j] = gram + jnp.where(lane == sub, ridge, 0.0)

    lane_row = lax.broadcasted_iota(jnp.int32, (1, rank), 1)

    @pl.loop(0, rank)
    def _(k):
        for j in range(len(pairs)):
            whole = inverse[j]
            row = inverse[j, pl.ds(k, 1), :]
            here = jnp.where(lane == k, whole, 0.0)
            column = jnp.sum(here, axis=1, keepdims=True)
            pivot = 1.0 / jnp.sum(jnp.where(lane_row == k, row, 0.0), axis=1, keepdims=True)
            scaled = jnp.where(lane_row == k, pivot, row * pivot)
            inverse[j] = jnp.where(lane == k, 0.0, whole) - column * scaled
            inverse[j, pl.ds(k, 1), :] = scaled

    for j, (block, chosen, out) in enumerate(pairs):
        cross = outer(block[...], chosen[...])
        out[...] = jnp.dot(
            cross, inverse[j], precision=HIGHEST, preferred_element_type=jnp.float32
        )


def partner(block, axis, apart):
    count = lax.axis_size(axis)
    route = []
    for low in range(count):
        high = low | 1 << apart
        if high != low and high < count:
            route += [(low, high), (high, low)]
    return lax.ppermute(block, axis, route)


def body(n, front, omega, leaf_pivots, pivots_one, pivots_two, pivots_three, pivots_four):
    rows_here = front.shape[0]
    width = omega.shape[1]
    samples = lax.psum(gather_matmul(front, omega, n), "col")
    leaf_count, rank = leaf_pivots.shape
    leaf_size = rows_here // leaf_count
    starts = leaf_size * jnp.arange(leaf_count, dtype=jnp.int32)[:, None]
    merged = jnp.take(samples, (leaf_pivots + starts).reshape(-1), axis=0)
    skeleton = jnp.take(merged, pivots_one[0], axis=0)
    skeletons = [skeleton]
    blocks = []
    position = lax.axis_index("row")
    for level, pivots in enumerate((pivots_two, pivots_three, pivots_four)):
        other = partner(skeleton, "row", level)
        lower = position >> level & 1 == 0
        block = jnp.where(
            lower, jnp.concatenate([skeleton, other], 0), jnp.concatenate([other, skeleton], 0)
        )
        node = position >> level + 1
        chosen_pivots = lax.dynamic_index_in_dim(pivots, node, 0, keepdims=False)
        skeleton = jnp.take(block, chosen_pivots, axis=0)
        blocks.append(block)
        skeletons.append(skeleton)
    problems = leaf_count + len(skeletons)
    basis = jax.ShapeDtypeStruct((1, leaf_size, rank), jnp.float32)
    outs = pl.pallas_call(
        functools.partial(interpolate_kernel, problems),
        out_shape=[jax.ShapeDtypeStruct((leaf_count, leaf_size, rank), jnp.float32)]
        + [basis] * len(skeletons),
        in_specs=[pl.BlockSpec(memory_space=pltpu.VMEM)] * 9,
        out_specs=[pl.BlockSpec(memory_space=pltpu.VMEM)] * 5,
        scratch_shapes=[pltpu.VMEM((problems, rank, rank), jnp.float32)],
    )(samples, merged, *blocks, *skeletons)
    return (samples, *outs)


def solution(mesh):
    in_specs = (
        P("row", "col"),
        P(("col", "row"), None),
        P("row", None),
        P("row", None),
        P(),
        P(),
        P(),
    )
    out_specs = (
        P("row", None),
        P("row", None, None),
        P("row", None, None),
        P("row", None, None),
        P("row", None, None),
        P("row", None, None),
    )
    return jax.shard_map(
        functools.partial(body, mesh.shape["row"]),
        mesh=mesh,
        in_specs=in_specs,
        out_specs=out_specs,
        check_vma=False,
    )
```

```python
import functools

import jax
import jax.numpy as jnp
from jax import lax
from jax.experimental import pallas as pl
from jax.experimental.pallas import tpu as pltpu
from jax.sharding import PartitionSpec as P

ridge = 1.0
MESH = pl.DeviceIdType.MESH
HIGHEST = lax.Precision.HIGHEST


def gather_matmul_kernel(
    n, stages, depth, pieces, front_ref, omega_ref, out_ref, held, cols, total, landed, whole,
    own_sem, front_sem, send_sem, recv_sem, sum_send, sum_recv
):
    half_ring = n // 2
    piece = depth // (2 * pieces)
    me = lax.axis_index("row")
    a, b = me // 2, me % 2
    spot = a + b * (n - 1 - 2 * a)

    def owner(place):
        place = (place + 2 * n) % n
        q = place // half_ring
        return 2 * (place + q * (n - 1 - 2 * place)) + q

    targets = (owner(spot + 1), owner(spot - 1))
    lane = lax.axis_index("col")
    sides = [(lane // (1 << t)) % 2 for t in range(stages)]
    mates = [lane + (1 << t) * (1 - 2 * sides[t]) for t in range(stages)]

    barrier = pltpu.get_barrier_semaphore()
    for target in targets:
        pl.semaphore_signal(barrier, inc=1, device_id={"row": target}, device_id_type=MESH)
    for mate in mates:
        pl.semaphore_signal(barrier, inc=1, device_id={"col": mate}, device_id_type=MESH)
    pl.semaphore_wait(barrier, 2 + stages)

    def rows_of(way, p):
        return pl.ds((way * pieces + p) * piece, piece)

    def source(step, way):
        return owner(spot - step) if way == 0 else owner(spot + step)

    def send(src, block, step, way, p):
        pltpu.make_async_remote_copy(
            src_ref=src,
            dst_ref=held.at[block, rows_of(way, p)],
            send_sem=send_sem.at[step, way, p],
            recv_sem=recv_sem.at[step, way, p],
            device_id={"row": targets[way]},
            device_id_type=MESH,
        ).start()

    def arrival(step, way, p):
        block = source(step + 1, way)
        rows = held.at[block, rows_of(way, p)]
        return pltpu.make_async_remote_copy(
            src_ref=rows,
            dst_ref=rows,
            send_sem=send_sem.at[step, way, p],
            recv_sem=recv_sem.at[step, way, p],
            device_id={"row": targets[way]},
            device_id_type=MESH,
        )

    def front_copy(block, way, p, slot):
        start = pl.multiple_of(block * depth + (way * pieces + p) * piece, piece)
        return pltpu.make_async_copy(
            front_ref.at[:, pl.ds(start, piece)], cols.at[slot], front_sem.at[slot]
        )

    for p in range(pieces):
        for way in range(2):
            send(omega_ref.at[rows_of(way, p)], me, 0, way, p)
    own = pltpu.make_async_copy(omega_ref, held.at[me], own_sem)
    own.start()
    for way in range(2):
        front_copy(me, way, 0, way).start()
    total[...] = jnp.zeros_like(total)
    own.wait()

    rows_tile = 256

    def multiply(block, way, p):
        @pl.loop(0, total.shape[0] // rows_tile)
        def _(i):
            tile = pl.ds(pl.multiple_of(i * rows_tile, rows_tile), rows_tile)
            total[tile, :] += jnp.dot(
                cols[way, tile, :],
                held[block, rows_of(way, p), :],
                precision=HIGHEST,
                preferred_element_type=jnp.float32,
            )

    def consume(step, p):
        for way in range(2):
            block = source(step, way)
            front_copy(block, way, p, way).wait()
            multiply(block, way, p)
            if p + 1 < pieces:
                front_copy(block, way, p + 1, way).start()
            else:

                @pl.when(step < n - 1)
                def _():
                    front_copy(source(step + 1, way), way, 0, way).start()

    for p in range(pieces):
        consume(0, p)

    @pl.loop(0, n - 1)
    def _(step):
        for p in range(pieces):
            for way in range(2):
                arrival(step, way, p).wait_recv()

                @pl.when(step < n - 2)
                def _():
                    block = source(step + 1, way)
                    send(held.at[block, rows_of(way, p)], block, step + 1, way, p)

            consume(step + 1, p)

    @pl.loop(0, n - 1)
    def _(step):
        for p in range(pieces):
            for way in range(2):
                arrival(step, way, p).wait_send()

    rows = total.shape[0]
    base = 0
    spans = []
    for t in range(stages):
        size = rows >> t + 1
        keep = pl.multiple_of(base + sides[t] * size, 8)
        give = pl.multiple_of(base + (1 - sides[t]) * size, 8)
        spans.append((keep, size))
        slot = landed.at[pl.ds(rows - (rows >> t), size)]
        copy = pltpu.make_async_remote_copy(
            src_ref=total.at[pl.ds(give, size)],
            dst_ref=slot,
            send_sem=sum_send.at[t],
            recv_sem=sum_recv.at[t],
            device_id={"col": mates[t]},
            device_id_type=MESH,
        )
        copy.start()
        copy.wait()
        total[pl.ds(keep, size), :] += slot[...]
        base = keep
    if stages:
        keep, size = spans[-1]
        whole[pl.ds(keep, size), :] = total[pl.ds(keep, size), :]
    else:
        whole[...] = total[...]
    for t in reversed(range(stages)):
        keep, size = spans[t]
        mine = whole.at[pl.ds(keep, size)]
        copy = pltpu.make_async_remote_copy(
            src_ref=mine,
            dst_ref=mine,
            send_sem=sum_send.at[stages + t],
            recv_sem=sum_recv.at[stages + t],
            device_id={"col": mates[t]},
            device_id_type=MESH,
        )
        copy.start()
        copy.wait()
    out_ref[...] = whole[...]


def gather_matmul(front, omega, n, stages):
    rows = front.shape[0]
    depth, width = omega.shape
    pieces = max(1, min(2, depth // 256))
    piece = depth // (2 * pieces)
    return pl.pallas_call(
        functools.partial(gather_matmul_kernel, n, stages, depth, pieces),
        out_shape=jax.ShapeDtypeStruct((rows, width), jnp.float32),
        in_specs=[pl.BlockSpec(memory_space=pl.ANY)] * 2,
        out_specs=pl.BlockSpec(memory_space=pltpu.VMEM),
        scratch_shapes=[
            pltpu.VMEM((n, depth, width), jnp.float32),
            pltpu.VMEM((2, rows, piece), jnp.float32),
            pltpu.VMEM((rows, width), jnp.float32),
            pltpu.VMEM((rows, width), jnp.float32),
            pltpu.VMEM((rows, width), jnp.float32),
            pltpu.SemaphoreType.DMA,
            pltpu.SemaphoreType.DMA((2,)),
            pltpu.SemaphoreType.DMA((n - 1, 2, pieces)),
            pltpu.SemaphoreType.DMA((n - 1, 2, pieces)),
            pltpu.SemaphoreType.DMA((2 * stages,)),
            pltpu.SemaphoreType.DMA((2 * stages,)),
        ],
        compiler_params=pltpu.CompilerParams(
            collective_id=0, has_side_effects=True, vmem_limit_bytes=60 * 1024 * 1024
        ),
    )(front, omega)


def interpolate_kernel(count, *refs):
    blocks, chosens, outs, inverses = [refs[i * count : (i + 1) * count] for i in range(4)]
    rank = outs[0].shape[2]

    def outer(x, y):
        return lax.dot_general(
            x, y, (((1,), (1,)), ((), ())), precision=HIGHEST, preferred_element_type=jnp.float32
        )

    lane = lax.broadcasted_iota(jnp.int32, (rank, rank), 1)
    sub = lax.broadcasted_iota(jnp.int32, (rank, rank), 0)
    lane_row = lax.broadcasted_iota(jnp.int32, (1, rank), 1)
    for chosen, inverse in zip(chosens, inverses):
        inverse[...] = outer(chosen[...], chosen[...]) + jnp.where(lane == sub, ridge, 0.0)

    def pick(values, at, index):
        return jnp.sum(jnp.where(at == index, values, 0.0), axis=1, keepdims=True)

    @pl.loop(0, rank // 2)
    def _(step):
        k = 2 * step
        wholes = [inverse[...] for inverse in inverses]
        firsts = [inverse[pl.ds(k, 1), :] for inverse in inverses]
        seconds = [inverse[pl.ds(k + 1, 1), :] for inverse in inverses]
        corners = [
            (pick(u, lane_row, k), pick(u, lane_row, k + 1), pick(v, lane_row, k), pick(v, lane_row, k + 1))
            for u, v in zip(firsts, seconds)
        ]
        lefts = [pick(whole, lane, k) for whole in wholes]
        rights = [pick(whole, lane, k + 1) for whole in wholes]
        news = []
        for (a, b, c, d), u, v in zip(corners, firsts, seconds):
            top = 1.0 / a
            beta = b * top
            s = jnp.where(lane_row == k, top, u * top)
            v1 = jnp.where(lane_row == k, 0.0, v) - c * s
            low = 1.0 / (d - c * beta)
            t = jnp.where(lane_row == k + 1, low, v1 * low)
            w = jnp.where(lane_row == k + 1, 0.0, s) - beta * t
            news.append((w, t))
        for inverse, whole, p, q, (w, t) in zip(inverses, wholes, lefts, rights, news):
            rest = jnp.where(lane // 2 == step, 0.0, whole) - p * w - q * t
            inverse[...] = jnp.where(sub == k, w, jnp.where(sub == k + 1, t, rest))

    for block, chosen, out, inverse in zip(blocks, chosens, outs, inverses):
        cross = outer(block[...], chosen[...])
        out[0] = jnp.dot(
            cross, inverse[...], precision=HIGHEST, preferred_element_type=jnp.float32
        )


def interpolate(blocks, chosens):
    count = len(blocks)
    leaf_size, width = blocks[0].shape
    rank = chosens[0].shape[0]
    basis = jax.ShapeDtypeStruct((1, leaf_size, rank), jnp.float32)
    return pl.pallas_call(
        functools.partial(interpolate_kernel, count),
        out_shape=[basis] * count,
        in_specs=[pl.BlockSpec(memory_space=pltpu.VMEM)] * (2 * count),
        out_specs=[pl.BlockSpec(memory_space=pltpu.VMEM)] * count,
        scratch_shapes=[pltpu.VMEM((rank, rank), jnp.float32)] * count,
        cost_estimate=pl.CostEstimate(
            flops=10**10, bytes_accessed=4 * count * (leaf_size + rank) * width, transcendentals=0
        ),
    )(*blocks, *chosens)


def partner(block, axis, apart):
    count = lax.axis_size(axis)
    route = []
    for low in range(count):
        high = low | 1 << apart
        if high != low and high < count:
            route += [(low, high), (high, low)]
    return lax.ppermute(block, axis, route)


def body(n, stages, front, omega, leaf_pivots, pivots_one, pivots_two, pivots_three, pivots_four):
    rows_here = front.shape[0]
    width = omega.shape[1]
    samples = gather_matmul(front, omega, n, stages)
    leaf_count, rank = leaf_pivots.shape
    leaf_size = rows_here // leaf_count
    starts = leaf_size * jnp.arange(leaf_count, dtype=jnp.int32)[:, None]
    merged = jnp.take(samples, (leaf_pivots + starts).reshape(-1), axis=0)
    skeleton = jnp.take(merged, pivots_one[0], axis=0)
    skeletons = [skeleton]
    blocks = []
    position = lax.axis_index("row")
    for level, pivots in enumerate((pivots_two, pivots_three, pivots_four)):
        other = partner(skeleton, "row", level)
        lower = position >> level & 1 == 0
        block = jnp.where(
            lower, jnp.concatenate([skeleton, other], 0), jnp.concatenate([other, skeleton], 0)
        )
        node = position >> level + 1
        chosen_pivots = lax.dynamic_index_in_dim(pivots, node, 0, keepdims=False)
        skeleton = jnp.take(block, chosen_pivots, axis=0)
        blocks.append(block)
        skeletons.append(skeleton)
    leaves = [samples[i * leaf_size : (i + 1) * leaf_size] for i in range(leaf_count)]
    chosens = [merged[i * rank : (i + 1) * rank] for i in range(leaf_count)]
    *leaf_basis, basis_one = interpolate(leaves + [merged], chosens + skeletons[:1])
    upper = interpolate(blocks, skeletons[1:])
    return (samples, jnp.concatenate(leaf_basis), basis_one, *upper)


def solution(mesh):
    in_specs = (
        P("row", "col"),
        P(("col", "row"), None),
        P("row", None),
        P("row", None),
        P(),
        P(),
        P(),
    )
    out_specs = (
        P("row", None),
        P("row", None, None),
        P("row", None, None),
        P("row", None, None),
        P("row", None, None),
        P("row", None, None),
    )
    return jax.shard_map(
        functools.partial(body, mesh.shape["row"], (mesh.shape["col"] - 1).bit_length()),
        mesh=mesh,
        in_specs=in_specs,
        out_specs=out_specs,
        check_vma=False,
    )
```
